128 devices in a mesh: groups: 4 (over y, x), seq: 16 (over z), head: 2 (over core).
Axes of the slice: x: 2, y: 2, z: 16, core: 2. Of those that a mesh axis runs over, the one named last changes fastest.
The devices are a block of a 8x8x16 slice.
Arguments:
- queries: bfloat16 [16384, 3584], P(('groups', 'seq'), 'head'), parts along dimension 0, may hold values from -30 to 30
- current_keys: bfloat16 [16384, 512], P(('groups', 'seq'), 'head'), parts along dimension 0, may hold values from -6 to 6
- current_values: bfloat16 [16384, 512], P(('groups', 'seq'), 'head'), parts along dimension 0, may hold values from -6 to 6
- stored_keys: bfloat16 [16384, 2, 512], P(('groups', 'seq'), None, 'head'), parts along dimension 0, may hold values from -22 to 22
- stored_values: bfloat16 [16384, 2, 512], P(('groups', 'seq'), None, 'head'), parts along dimension 0, may hold values from -6 to 6
- remap_table: int32 [3, 256], P(None, ('groups', 'seq')), parts along dimension 1, may hold values from 0 to 4095
- block_table: int32 [1024], P('groups'), parts along dimension 0, may hold values from 0 to 15, as said below
Outputs:
- attended: bfloat16 [16384, 3584], P(('groups', 'seq'), 'head'), parts along dimension 0
- paged_keys: bfloat16 [4, 1024, 2048], P('head', ('groups', 'seq')), parts along dimension 1
- paged_values: bfloat16 [4, 1024, 2048], P('head', ('groups', 'seq')), parts along dimension 1
The draws below stay inside these ranges and needn't reach their ends.
There are 4 independent parts, one for each index of `groups`. The reference program is written for one: setup_inputs(seed, part) draws one part's arguments, and reference() takes and returns one part's arrays. A program takes and returns all parts, laid end to end along the dimension named above; each array names one. Nothing has to cross between parts.
Inputs may be any that keep to these rules, and one draw needn't show every extreme that they name: `block_table`: the entries of the blocks b that share b modulo 16 are a permutation of 0 to 15.
All inputs are finite; a program needn't handle non-finite values.
Results may differ from the reference program's by a relative error of at most 0.012.
The reference program's roundings to bfloat16 on the way count: a program that leaves them out, or rounds other values in their place, can miss the bound.
Values may be sent and summed in bfloat16 or wider, within the bound.
No kernel may reach another device: no remote copies, remote signals or barrier semaphores. Data moves between devices by JAX's collectives and lax.ppermute only.
A program may use at most 128 MiB of HBM per device.

```python
import jax
import jax.numpy as jnp
from jax import lax

HQ = 28
KEY_VALUE_HEADS = 4
HEAD_SIZE = 128
PRIOR_SEGMENTS = 2
PAGE_TOKENS = 16
QBLK = 64
QUERY_PER_KEY = 7
SEGMENT_TOKENS = 4096
NQB = 64
SEGMENT_PAGES = 256
OWNERS = 16
PAGES_DEV = 16


def draw_queries(key, part):
    rotary_base = jnp.clip(jax.random.normal(jax.random.fold_in(key, 1), (SEGMENT_TOKENS, HQ * HEAD_SIZE), jnp.float32), -6.0, 6.0) * 2.2
    return rotary_base.astype(jnp.bfloat16)


def draw_stored_keys(key, part):
    rotary_base = jnp.clip(jax.random.normal(jax.random.fold_in(key, 2), (SEGMENT_TOKENS, PRIOR_SEGMENTS, KEY_VALUE_HEADS * HEAD_SIZE), jnp.float32), -6.0, 6.0)
    return rotary_base.astype(jnp.bfloat16)


def draw_block_table(key, part):
    holder_keys = jax.random.split(jax.random.fold_in(key, 5), OWNERS)
    orders = jax.vmap(lambda single: jax.random.permutation(single, PAGES_DEV))(holder_keys)
    return orders.T.reshape(-1).astype(jnp.int32)


def touch_ends(entries, own_key, smallest, top_value):
    spot = [jax.random.randint(jax.random.fold_in(own_key, axis), (), 0, length) for axis, length in enumerate(entries.shape)]
    main_axis = entries.shape.index(max(entries.shape))
    beside = spot[:main_axis] + [(spot[main_axis] + 1) % entries.shape[main_axis]] + spot[main_axis + 1:]
    return entries.at[tuple(spot)].set(smallest).at[tuple(beside)].set(top_value)


def block_levels(own_key, dims, cuts, least, top_value):
    def one(dim, shards_of):
        steps = jax.random.uniform(jax.random.fold_in(jax.random.fold_in(own_key, 6), dim), (shards_of,), jnp.float32, least / len(cuts), top_value / len(cuts))
        return jnp.repeat(jnp.exp(steps), dims[dim] // shards_of).reshape((-1,) + (1,) * (len(dims) - dim - 1))

    gain = one(*cuts[0])
    for cut in cuts[1:]:
        gain = gain * one(*cut)
    return gain


def scatter_about(stream_key, extent, spread, most, cuts=(), kind=jnp.bfloat16):
    loudness = block_levels(stream_key, extent, cuts, -0.22, 0.18) if cuts else 1.0
    values = jax.random.normal(stream_key, extent, jnp.float32) * spread * loudness
    return jnp.minimum(jnp.maximum(values, -most), most).astype(kind)


def setup_inputs(seed: int = 0, part: int = 0) -> dict:
    key_list = jax.random.split(jax.random.key(seed), 8)
    part_splits = jax.random.split(jax.random.fold_in(key_list[7], part), 8)
    queries = draw_queries(jax.random.fold_in(jax.random.fold_in(key_list[7], part), 71), part)
    current_keys = scatter_about(part_splits[1], (SEGMENT_TOKENS, KEY_VALUE_HEADS * HEAD_SIZE), 1.0, 6.0, ((0, 16), (1, 2)))
    current_values = scatter_about(part_splits[2], (SEGMENT_TOKENS, KEY_VALUE_HEADS * HEAD_SIZE), 1.0, 6.0, ((0, 16), (1, 2)))
    stored_keys = draw_stored_keys(jax.random.fold_in(jax.random.fold_in(key_list[7], part), 71), part)
    stored_values = scatter_about(part_splits[4], (SEGMENT_TOKENS, PRIOR_SEGMENTS, KEY_VALUE_HEADS * HEAD_SIZE), 1.0, 6.0, ((0, 16), (2, 2)))
    remap_table = touch_ends(jax.random.randint(part_splits[5], (3, NQB), 0, SEGMENT_TOKENS), jax.random.fold_in(part_splits[5], 1), 0, SEGMENT_TOKENS - 1).astype(jnp.int32)
    block_table = draw_block_table(jax.random.fold_in(jax.random.fold_in(key_list[7], part), 71), part)
    return dict(queries=queries, current_keys=current_keys, current_values=current_values, stored_keys=stored_keys, stored_values=stored_values, remap_table=remap_table, block_table=block_table)


rope_base = 1000000.0
masked_value = -1e30


def apply_rotary(values, token_positions):
    half_dim = values.shape[-1] // 2
    frequency = rope_base ** (-2.0 * jnp.arange(half_dim, dtype=jnp.float32) / values.shape[-1])
    angles = token_positions.astype(jnp.float32)[:, None] * frequency[None, :]
    cos_table = jnp.cos(angles)[:, None, :]
    sin_table = jnp.sin(angles)[:, None, :]
    first_half = values[..., :half_dim]
    second_half = values[..., half_dim:]
    return jnp.concatenate([first_half * cos_table - second_half * sin_table, second_half * cos_table + first_half * sin_table], -1)


def paged_layout(cache_portion, block_table):
    page_blocks = cache_portion.reshape(SEGMENT_PAGES, PAGE_TOKENS, KEY_VALUE_HEADS, HEAD_SIZE).transpose(2, 0, 1, 3).reshape(KEY_VALUE_HEADS, SEGMENT_PAGES, PAGE_TOKENS * HEAD_SIZE)
    block_index = jnp.arange(SEGMENT_PAGES, dtype=jnp.int32)
    target = (block_index % OWNERS) * PAGES_DEV + block_table
    return jnp.zeros_like(page_blocks).at[:, target].set(page_blocks)


def reference(queries, current_keys, current_values, stored_keys, stored_values, remap_table, block_table):
    token_index = jnp.arange(SEGMENT_TOKENS, dtype=jnp.int32)
    token_positions = jnp.repeat(remap_table, QBLK, axis=1) + (token_index % QBLK)[None, :]
    query_single_float = queries.astype(jnp.float32).reshape(SEGMENT_TOKENS, HQ, HEAD_SIZE)
    rotary_output = [apply_rotary(query_single_float, token_positions[segment_kind_index]).astype(jnp.bfloat16).reshape(SEGMENT_TOKENS, KEY_VALUE_HEADS, QUERY_PER_KEY, HEAD_SIZE) for segment_kind_index in range(3)]
    score_scale = HEAD_SIZE ** -0.5
    value_portions = [stored_values[:, segment_number, :] for segment_number in range(PRIOR_SEGMENTS)] + [current_values]
    joined_values = jnp.concatenate(value_portions, 0).reshape((PRIOR_SEGMENTS + 1) * SEGMENT_TOKENS, KEY_VALUE_HEADS, HEAD_SIZE).astype(jnp.float32)
    query_block = min(256, SEGMENT_TOKENS)

    def one_block(block_number):
        first_row = block_number * query_block
        score_parts = []
        for segment_number in range(PRIOR_SEGMENTS):
            chosen = rotary_output[2] if segment_number < PRIOR_SEGMENTS - 1 else rotary_output[1]
            query_rows = lax.dynamic_slice_in_dim(chosen, first_row, query_block, 0).astype(jnp.float32)
            key_row_list = stored_keys[:, segment_number, :].reshape(SEGMENT_TOKENS, KEY_VALUE_HEADS, HEAD_SIZE).astype(jnp.float32)
            score_parts.append(jnp.einsum("qgrd,kgd->grqk", query_rows, key_row_list) * score_scale)
        query_rows = lax.dynamic_slice_in_dim(rotary_output[0], first_row, query_block, 0).astype(jnp.float32)
        key_row_list = current_keys.reshape(SEGMENT_TOKENS, KEY_VALUE_HEADS, HEAD_SIZE).astype(jnp.float32)
        intra = jnp.einsum("qgrd,kgd->grqk", query_rows, key_row_list) * score_scale
        allowed = token_index[None, :] <= (first_row + jnp.arange(query_block, dtype=jnp.int32))[:, None]
        score_parts.append(jnp.where(allowed[None, None], intra, masked_value))
        scores = jnp.concatenate(score_parts, -1)
        weights = jnp.exp(scores - jnp.max(scores, -1, keepdims=True))
        denom = jnp.sum(weights, -1)
        rounded = weights.astype(jnp.bfloat16).astype(jnp.float32)
        summed = jnp.einsum("grqk,kgd->qgrd", rounded, joined_values)
        result = summed / denom.transpose(2, 0, 1)[..., None]
        return result.astype(jnp.bfloat16).reshape(query_block, HQ * HEAD_SIZE)

    attended = lax.map(one_block, jnp.arange(SEGMENT_TOKENS // query_block, dtype=jnp.int32)).reshape(SEGMENT_TOKENS, HQ * HEAD_SIZE)
    paged_keys = paged_layout(stored_keys[:, PRIOR_SEGMENTS - 1, :], block_table)
    paged_values = paged_layout(stored_values[:, PRIOR_SEGMENTS - 1, :], block_table)
    return (attended, paged_keys, paged_values)
```

```python
import functools
import math

import jax
import jax.numpy as jnp
from jax import lax
from jax.experimental import pallas as pl
from jax.experimental.pallas import tpu as pltpu
from jax.sharding import PartitionSpec as P


HEAD_SIZE = 128
PRIOR_SEGMENTS = 2
PAGE_TOKENS = 16
QBLK = 64

rope_base = 1000000.0
masked_value = -1e30
EXP2_SCALE = math.log2(math.e) / math.sqrt(HEAD_SIZE)

ONES = 16
VMEM_LIMIT = 40 * 1024 * 1024


def rotate_kernel(cos_ref, sin_ref, qa_ref, qb_ref, out_ref):
    for g, ref in enumerate((qa_ref, qb_ref)):
        x = ref[...].astype(jnp.float32)
        swapped = pltpu.roll(x, HEAD_SIZE // 2, 1)
        for kind in range(3):
            out_ref[g, kind, 0] = (x * cos_ref[kind] + swapped * sin_ref[kind]).astype(jnp.bfloat16)


def rotate_queries(queries, remap_table, kv_local, per_group):
    rows = queries.shape[0]
    half = HEAD_SIZE // 2
    positions = (
        jnp.repeat(remap_table, QBLK, axis=1)
        + (jnp.arange(rows, dtype=jnp.int32) % QBLK)[None, :]
    )
    frequency = rope_base ** (-2.0 * jnp.arange(half, dtype=jnp.float32) / HEAD_SIZE)
    angles = positions.astype(jnp.float32)[:, :, None] * frequency[None, None, :]
    cos, sin = jnp.cos(angles), jnp.sin(angles)
    cos = jnp.concatenate([cos, cos], -1)
    sin = jnp.concatenate([-sin, sin], -1)
    table = pl.BlockSpec((3, rows, HEAD_SIZE), lambda r: (0, 0, 0))
    return pl.pallas_call(
        rotate_kernel,
        grid=(per_group,),
        in_specs=[
            table,
            table,
            pl.BlockSpec((rows, HEAD_SIZE), lambda r: (0, r)),
            pl.BlockSpec((rows, HEAD_SIZE), lambda r: (0, per_group + r)),
        ],
        out_specs=pl.BlockSpec(
            (kv_local, 3, 1, rows, HEAD_SIZE), lambda r: (0, 0, r, 0, 0)
        ),
        out_shape=jax.ShapeDtypeStruct(
            (kv_local, 3, per_group, rows, HEAD_SIZE), jnp.bfloat16
        ),
        name="rotate",
        cost_estimate=pl.CostEstimate(flops=4_000_000_000, bytes_accessed=4_000_000, transcendentals=0),
    )(cos, sin, queries, queries)


def score(g, r, parts, max_ref, score_ref):
    best = []
    for n, (k, q, mask) in enumerate(parts):
        s = lax.dot_general(k, q, (((1,), (1,)), ((), ())), preferred_element_type=jnp.float32)
        if mask is not None:
            s = jnp.where(mask, s, masked_value)
        score_ref[n * s.shape[0] : (n + 1) * s.shape[0]] = s
        best.append(jnp.max(s, axis=0, keepdims=True))
    old_max = max_ref[g, r]
    new_max = functools.reduce(jnp.maximum, best, old_max)
    max_ref[g, r] = new_max
    return new_max, jnp.exp2((old_max - new_max) * EXP2_SCALE)


def weigh(keys, new_max, score_ref, weight_ref):
    weight_ref[:keys] = jnp.exp2((score_ref[:keys] - new_max) * EXP2_SCALE).astype(jnp.bfloat16)


def collect(g, r, keys, values, factor, weight_ref, acc_ref):
    product = jnp.dot(values, weight_ref[:keys], preferred_element_type=jnp.float32)
    acc_ref[g, r] = acc_ref[g, r] * factor + product


def put_page(page_ref, g, kv_ref, place, slot):
    for which in range(2):
        page_ref[g, which, slot] = kv_ref[
            PRIOR_SEGMENTS - 1, which, pl.ds(pl.multiple_of(place * PAGE_TOKENS, PAGE_TOKENS), PAGE_TOKENS), :
        ]


def attend_kernel(hops, owners, kv_local, first, last, info_ref, *refs):
    count = len(hops)
    q_ref, refs = refs[0], refs[1:]
    kv_refs, refs = refs[: kv_local * count], refs[kv_local * count :]
    if not first:
        acc_ref, max_ref, page_ref = refs[:3]
        refs = refs[3:] if last else refs[6:]
    if first:
        acc_ref, max_ref, page_ref = refs[:3]
        refs = refs[3:]
    if last:
        out_ref, page_key_ref, page_value_ref = refs[:3]
        refs = refs[3:]
    if not last:
        refs[0][...] = jnp.zeros_like(refs[0])
        refs = refs[1:]
    turned_ref, score_a, score_b, weight_a, weight_b = refs
    _, _, per_group, rows, _ = q_ref.shape
    me = info_ref[owners]
    sources = [lax.rem(me + owners - hop, owners) for hop in hops]

    if first:
        acc_ref[...] = jnp.zeros_like(acc_ref)
        max_ref[...] = jnp.full_like(max_ref, masked_value)
    for g in range(kv_local):
        for c in range(count):
            put_page(page_ref, g, kv_refs[g * count + c], me, info_ref[sources[c]])
            for segment in range(PRIOR_SEGMENTS + 1):
                turned_ref[g * count + c, segment, :HEAD_SIZE] = kv_refs[g * count + c][segment, 1].T
                turned_ref[g * count + c, segment, HEAD_SIZE:] = jnp.ones((ONES, rows), jnp.bfloat16)

    def run(which, segments, mask=None):
        keys = len(which) * len(segments) * rows

        def parts(g, r):
            return [
                (kv_refs[g * count + c][segment, 0], q_ref[g, kind, r], mask)
                for segment, kind in segments
                for c in which
            ]

        def values(g):
            return jnp.concatenate(
                [turned_ref[g * count + c, segment] for segment, _ in segments for c in which], axis=1
            )

        def step(r, carry):
            max_a, factor_a, factor_b = carry
            max_b, next_b = score(1, r, parts(1, r), max_ref, score_b)
            weigh(keys, max_a, score_a, weight_a)
            collect(1, jnp.maximum(r - 1, 0), keys, values(1), factor_b, weight_b, acc_ref)
            following = jnp.minimum(r + 1, per_group - 1)
            next_a = score(0, following, parts(0, following), max_ref, score_a)
            weigh(keys, max_b, score_b, weight_b)
            collect(0, r, keys, values(0), factor_a, weight_a, acc_ref)
            return (*next_a, next_b)

        weight_b[:keys] = jnp.zeros((keys, rows), jnp.bfloat16)
        start = score(0, 0, parts(0, 0), max_ref, score_a)
        _, _, factor_b = lax.fori_loop(0, per_group, step, (*start, jnp.ones((1, rows), jnp.float32)))
        collect(1, per_group - 1, keys, values(1), factor_b, weight_b, acc_ref)

    stored = [(n, 2 if n < PRIOR_SEGMENTS - 1 else 1) for n in range(PRIOR_SEGMENTS)]
    current = [(PRIOR_SEGMENTS, 0)]
    run(range(count), stored)
    if first:
        shape = (rows, rows)
        mask = lax.broadcasted_iota(jnp.int32, shape, 0) <= lax.broadcasted_iota(jnp.int32, shape, 1)
        run([0], current, mask)
    elif count == 1:

        @pl.when(sources[0] < me)
        def before():
            run([0], current)

    else:
        @pl.when((sources[0] < me) & (sources[1] > me))
        def one():
            run([0], current)

        @pl.when(sources[1] < me)
        def two():
            run([0, 1], current)

    if last:
        @pl.loop(0, per_group)
        def finish(r):
            for g in range(kv_local):
                column = pl.multiple_of((g * per_group + r) * HEAD_SIZE, HEAD_SIZE)
                out_ref[:, pl.ds(column, HEAD_SIZE)] = (acc_ref[g, r, :HEAD_SIZE] / acc_ref[g, r, HEAD_SIZE : HEAD_SIZE + 1]).T.astype(jnp.bfloat16)

        for g in range(kv_local):
            for which, ref in enumerate((page_key_ref, page_value_ref)):
                tokens = page_ref[g, which].astype(jnp.float32)
                for t in range(PAGE_TOKENS):
                    ref[g, :, t * HEAD_SIZE : (t + 1) * HEAD_SIZE] = tokens[:, t, :].astype(jnp.bfloat16)


def attend(info, q, chunks, state, hops, owners, first=False, last=False):
    kv_local, _, per_group, rows, _ = q.shape
    flat = [c for of_head in chunks for c in of_head]
    pages = rows // PAGE_TOKENS
    whole = pl.BlockSpec(memory_space=pltpu.VMEM)
    operands = [info, q, *flat]
    aliases = {}
    if not first:
        if not last:
            aliases = {len(operands) + n: n for n in range(3)}
        operands += state
    if last:
        page = jax.ShapeDtypeStruct((kv_local, pages, PAGE_TOKENS * HEAD_SIZE), jnp.bfloat16)
        width = kv_local * per_group * HEAD_SIZE
        out_shape = [jax.ShapeDtypeStruct((rows, width), jnp.bfloat16), page, page]
    else:
        out_shape = [
            *[
                jax.ShapeDtypeStruct((kv_local, per_group, n, rows), jnp.float32)
                for n in (HEAD_SIZE + ONES, 1)
            ],
            jax.ShapeDtypeStruct((kv_local, 2, pages, PAGE_TOKENS, HEAD_SIZE), jnp.bfloat16),
            jax.ShapeDtypeStruct((8, HEAD_SIZE), jnp.float32),
        ]
    return pl.pallas_call(
        functools.partial(attend_kernel, hops, owners, kv_local, first, last),
        in_specs=[pl.BlockSpec(memory_space=pltpu.SMEM)] + [whole] * (len(operands) - 1),
        out_specs=[whole] * len(out_shape),
        out_shape=out_shape,
        scratch_shapes=[
            pltpu.VMEM((len(flat), PRIOR_SEGMENTS + 1, HEAD_SIZE + ONES, rows), jnp.bfloat16),
            *[pltpu.VMEM((len(hops) * PRIOR_SEGMENTS * rows, rows), t) for t in (jnp.float32, jnp.float32, jnp.bfloat16, jnp.bfloat16)],
        ],
        input_output_aliases=aliases,
        compiler_params=pltpu.CompilerParams(vmem_limit_bytes=VMEM_LIMIT),
        name="attend",
        cost_estimate=pl.CostEstimate(
            flops=4 * len(hops) * kv_local * per_group * rows * rows * 3 * HEAD_SIZE,
            bytes_accessed=10_000_000,
            transcendentals=len(hops) * kv_local * per_group * rows * rows * 3,
        ),
    )(*operands)


def shards(
    queries, current_keys, current_values, stored_keys, stored_values, remap_table, block_table
):
    rows = queries.shape[0]
    kv_local = current_keys.shape[1] // HEAD_SIZE
    per_group = queries.shape[1] // (kv_local * HEAD_SIZE)
    owners = lax.axis_size("seq")
    me = lax.axis_index("seq")
    right = [(i, (i + 1) % owners) for i in range(owners)]
    left = [(i, (i - 1) % owners) for i in range(owners)]

    def packed(g):
        columns = slice(g * HEAD_SIZE, (g + 1) * HEAD_SIZE)
        stored = jnp.stack([stored_keys[:, :, columns], stored_values[:, :, columns]]).transpose(2, 0, 1, 3)
        current = jnp.stack([current_keys[:, columns], current_values[:, columns]])[None]
        return jnp.concatenate([stored, current])

    own = [packed(g) for g in range(kv_local)]
    slots = lax.dynamic_slice_in_dim(block_table.reshape(owners, owners), me, 1, 1)[:, 0]
    info = jnp.concatenate([slots, me[None].astype(jnp.int32)])

    q = rotate_queries(queries, remap_table, kv_local, per_group)
    rightward, leftward = list(own), list(own)
    state = None
    for hop in range(1, owners // 2 + 1):
        held = [[rightward[g], leftward[g]] for g in range(kv_local)]
        if state is not None:
            for g in range(kv_local):
                rightward[g], leftward[g], _ = lax.optimization_barrier((rightward[g], leftward[g], mark))
        if hop < owners // 2:
            for g in range(kv_local):
                rightward[g] = lax.ppermute(rightward[g], "seq", right)
                leftward[g] = lax.ppermute(leftward[g], "seq", left)
        else:
            far = [
                lax.ppermute(rightward[g], "seq", right) if g % 2 == 0 else lax.ppermute(leftward[g], "seq", left)
                for g in range(kv_local)
            ]
        if state is None:
            *state, mark = attend(info, q, [[c] for c in own], None, (0,), owners, first=True)
        else:
            *state, mark = attend(info, q, held, state, (hop - 1, owners - hop + 1), owners)
    return tuple(attend(info, q, [[c] for c in far], state, (owners // 2,), owners, last=True))


def solution(mesh):
    in_specs = (
        P(("groups", "seq"), "head"),
        P(("groups", "seq"), "head"),
        P(("groups", "seq"), "head"),
        P(("groups", "seq"), None, "head"),
        P(("groups", "seq"), None, "head"),
        P(None, ("groups", "seq")),
        P("groups"),
    )
    out_specs = (
        P(("groups", "seq"), "head"),
        P("head", ("groups", "seq"), None),
        P("head", ("groups", "seq"), None),
    )
    return jax.shard_map(shards, mesh=mesh, in_specs=in_specs, out_specs=out_specs, check_vma=False)
```

```python
import functools
import math

import jax
import jax.numpy as jnp
from jax import lax
from jax.experimental import pallas as pl
from jax.experimental.pallas import tpu as pltpu
from jax.sharding import PartitionSpec as P


HEAD_SIZE = 128
PRIOR_SEGMENTS = 2
PAGE_TOKENS = 16
QBLK = 64

rope_base = 1000000.0
masked_value = -1e30
EXP2_SCALE = math.log2(math.e) / math.sqrt(HEAD_SIZE)

ONES = 16
WHOLE = pl.BlockSpec(memory_space=pltpu.VMEM)
VMEM_LIMIT = 40 * 1024 * 1024


def rotate_kernel(cos_ref, sin_ref, query_ref, out_ref, wide_cos, wide_sin):
    kv_local, kinds, per_group, _, _ = out_ref.shape
    for kind in range(kinds):
        wide_cos[kind] = jnp.concatenate([cos_ref[kind], cos_ref[kind]], -1)
        wide_sin[kind] = jnp.concatenate([-sin_ref[kind], sin_ref[kind]], -1)

    @pl.loop(0, per_group)
    def of_head(r):
        for g in range(kv_local):
            column = pl.multiple_of((g * per_group + r) * HEAD_SIZE, HEAD_SIZE)
            x = query_ref[:, pl.ds(column, HEAD_SIZE)].astype(jnp.float32)
            swapped = pltpu.roll(x, HEAD_SIZE // 2, 1)
            for kind in range(kinds):
                out_ref[g, kind, r] = (x * wide_cos[kind] + swapped * wide_sin[kind]).astype(jnp.bfloat16)


def rotate_queries(queries, remap_table, kv_local, per_group):
    rows = queries.shape[0]
    half = HEAD_SIZE // 2
    positions = (
        jnp.repeat(remap_table, QBLK, axis=1)
        + (jnp.arange(rows, dtype=jnp.int32) % QBLK)[None, :]
    )
    frequency = rope_base ** (-2.0 * jnp.arange(half, dtype=jnp.float32) / HEAD_SIZE)
    angles = positions.astype(jnp.float32)[:, :, None] * frequency[None, None, :]
    return pl.pallas_call(
        rotate_kernel,
        in_specs=[WHOLE] * 3,
        out_specs=WHOLE,
        out_shape=jax.ShapeDtypeStruct((kv_local, 3, per_group, rows, HEAD_SIZE), jnp.bfloat16),
        scratch_shapes=[pltpu.VMEM((3, rows, HEAD_SIZE), jnp.float32)] * 2,
        compiler_params=pltpu.CompilerParams(vmem_limit_bytes=16 * 1024 * 1024),
        name="rotate",
        cost_estimate=pl.CostEstimate(flops=1_000_000_000, bytes_accessed=4_000_000, transcendentals=0),
    )(jnp.cos(angles), jnp.sin(angles), queries)


def score(g, r, parts, max_ref, score_ref):
    best = []
    for n, (k, q, mask) in enumerate(parts):
        s = lax.dot_general(k, q, (((1,), (1,)), ((), ())), preferred_element_type=jnp.float32)
        if mask is not None:
            s = jnp.where(mask, s, masked_value)
        score_ref[n * s.shape[0] : (n + 1) * s.shape[0]] = s
        best.append(jnp.max(s, axis=0, keepdims=True))
    old_max = max_ref[g, r]
    new_max = functools.reduce(jnp.maximum, best, old_max)
    max_ref[g, r] = new_max
    return new_max, jnp.exp2((old_max - new_max) * EXP2_SCALE)


def weigh(keys, new_max, score_ref, weight_ref):
    weight_ref[:keys] = jnp.exp2((score_ref[:keys] - new_max) * EXP2_SCALE).astype(jnp.bfloat16)


def collect(g, r, keys, values, factor, weight_ref, acc_ref):
    product = jnp.dot(values, weight_ref[:keys], preferred_element_type=jnp.float32)
    acc_ref[g, r] = acc_ref[g, r] * factor + product


def put_page(page_ref, g, kv_ref, place, source):
    for which in range(2):
        page_ref[g, which, source] = kv_ref[
            PRIOR_SEGMENTS - 1, which, pl.ds(pl.multiple_of(place * PAGE_TOKENS, PAGE_TOKENS), PAGE_TOKENS), :
        ]


def attend_kernel(hops, owners, kv_local, stage, *refs):
    count = len(hops)
    if stage == "stored":
        slot_ref, refs = refs[0], refs[1:]
    q_ref, refs = refs[0], refs[1:]
    kv_refs, refs = refs[: kv_local * count], refs[kv_local * count :]
    _, _, per_group, rows, _ = q_ref.shape
    if stage == "first":
        (acc_ref, max_ref, page_ref), refs = refs[:3], refs[3:]
    elif stage == "middle":
        (acc_ref, max_ref, page_ref), refs = refs[:3], refs[6:]
    elif stage == "stored":
        (acc_ref, max_ref, page_ref), refs = refs[:3], refs[6:]
        (page_key_ref, page_value_ref, *refs, place_ref) = refs
    else:
        (acc_ref, max_ref), refs = refs[:2], refs[4:]
        (out_ref, *refs) = refs
    turned_ref, score_refs, weight_refs = refs[0], refs[1 : 1 + kv_local], refs[1 + kv_local :]
    me = lax.axis_index("seq")
    sources = [lax.rem(me + owners - hop, owners) for hop in hops]
    held = {
        "first": range(PRIOR_SEGMENTS + 1),
        "middle": range(PRIOR_SEGMENTS + 1),
        "stored": range(PRIOR_SEGMENTS),
        "finish": range(PRIOR_SEGMENTS, PRIOR_SEGMENTS + 1),
    }[stage]
    base = held[0]

    if stage == "first":
        acc_ref[...] = jnp.zeros_like(acc_ref)
        max_ref[...] = jnp.full_like(max_ref, masked_value)
    for g in range(kv_local):
        for c in range(count):
            kv = kv_refs[g * count + c]
            if stage != "finish":
                put_page(page_ref, g, kv, me, sources[c])
            for segment in held:
                turned_ref[g * count + c, segment, :HEAD_SIZE] = kv[segment - base, 1].T
                turned_ref[g * count + c, segment, HEAD_SIZE:] = jnp.ones((ONES, rows), jnp.bfloat16)

    def run(which, segments, mask=None):
        keys = len(which) * len(segments) * rows

        def parts(g, r):
            return [
                (kv_refs[g * count + c][segment - base, 0], q_ref[g, kind, r], mask)
                for segment, kind in segments
                for c in which
            ]

        def values(g):
            return jnp.concatenate(
                [turned_ref[g * count + c, segment] for segment, _ in segments for c in which], axis=1
            )

        heads = range(kv_local)

        def step(r, carry):
            maxima, factors = carry
            for g in heads:
                collect(g, jnp.maximum(r - 1, 0), keys, values(g), factors[g], weight_refs[g], acc_ref)
            following = jnp.minimum(r + 1, per_group - 1)
            scored = []
            for g in heads:
                weigh(keys, maxima[g][0], score_refs[g], weight_refs[g])
                scored.append(score(g, following, parts(g, following), max_ref, score_refs[g]))
            return scored, [of_head[1] for of_head in maxima]

        for g in heads:
            weight_refs[g][:keys] = jnp.zeros((keys, rows), jnp.bfloat16)
        scored = [score(g, 0, parts(g, 0), max_ref, score_refs[g]) for g in heads]
        _, factors = lax.fori_loop(0, per_group, step, (scored, [jnp.ones((1, rows), jnp.float32) for _ in heads]))
        for g in heads:
            collect(g, per_group - 1, keys, values(g), factors[g], weight_refs[g], acc_ref)

    stored = [(n, 2 if n < PRIOR_SEGMENTS - 1 else 1) for n in range(PRIOR_SEGMENTS)]
    current = [(PRIOR_SEGMENTS, 0)]
    if stage != "finish":
        run(range(count), stored)
    if stage == "first":
        shape = (rows, rows)
        mask = lax.broadcasted_iota(jnp.int32, shape, 0) <= lax.broadcasted_iota(jnp.int32, shape, 1)
        run([0], current, mask)
    elif stage == "finish":

        @pl.when(sources[0] < me)
        def before():
            run([0], current)

        @pl.loop(0, per_group)
        def finish(r):
            for g in range(kv_local):
                column = pl.multiple_of((g * per_group + r) * HEAD_SIZE, HEAD_SIZE)
                out_ref[:, pl.ds(column, HEAD_SIZE)] = (
                    (acc_ref[g, r, :HEAD_SIZE] / acc_ref[g, r, HEAD_SIZE : HEAD_SIZE + 1]).T.astype(jnp.bfloat16)
                )

    elif stage == "middle":
        @pl.when((sources[0] < me) & (sources[1] > me))
        def one():
            run([0], current)

        @pl.when(sources[1] < me)
        def two():
            run([0, 1], current)

    else:
        for source in range(owners):
            for g in range(kv_local):
                for which in range(2):
                    place_ref[g, which, slot_ref[source]] = page_ref[g, which, source]
        for g in range(kv_local):
            for which, ref in enumerate((page_key_ref, page_value_ref)):
                tokens = place_ref[g, which].astype(jnp.float32)
                for t in range(PAGE_TOKENS):
                    ref[g, :, t * HEAD_SIZE : (t + 1) * HEAD_SIZE] = tokens[:, t, :].astype(jnp.bfloat16)


def attend(q, chunks, state, hops, owners, stage, slots=None):
    kv_local, _, per_group, rows, _ = q.shape
    flat = [c for of_head in chunks for c in of_head]
    pages = rows // PAGE_TOKENS
    operands = [q, *flat] if slots is None else [slots, q, *flat]
    aliases = {len(operands) + n: n for n in range(len(state))}
    operands += state
    states = [
        jax.ShapeDtypeStruct((kv_local, per_group, n, rows), jnp.float32) for n in (HEAD_SIZE + ONES, 1)
    ]
    held_pages = jax.ShapeDtypeStruct((kv_local, 2, pages, PAGE_TOKENS, HEAD_SIZE), jnp.bfloat16)
    page = jax.ShapeDtypeStruct((kv_local, pages, PAGE_TOKENS * HEAD_SIZE), jnp.bfloat16)
    if stage == "finish":
        out_shape = [*states, jax.ShapeDtypeStruct((rows, kv_local * per_group * HEAD_SIZE), jnp.bfloat16)]
    elif stage == "stored":
        out_shape = [*states, held_pages, page, page]
    else:
        out_shape = [
            *states,
            held_pages,
        ]
    segments = {"first": 3, "middle": 3, "stored": 2, "finish": 1}[stage]
    keys = len(hops) * rows * (1 if stage == "finish" else PRIOR_SEGMENTS)
    pairs = len(hops) * kv_local * per_group * rows * rows * segments
    return pl.pallas_call(
        functools.partial(attend_kernel, hops, owners, kv_local, stage),
        in_specs=[pl.BlockSpec(memory_space=pltpu.SMEM)] * (slots is not None) + [WHOLE] * (len(operands) - (slots is not None)),
        out_specs=[WHOLE] * len(out_shape),
        out_shape=out_shape,
        scratch_shapes=[
            pltpu.VMEM((len(flat), PRIOR_SEGMENTS + 1, HEAD_SIZE + ONES, rows), jnp.bfloat16),
            *[pltpu.VMEM((keys, rows), t) for t in [jnp.float32] * kv_local + [jnp.bfloat16] * kv_local],
            *[pltpu.VMEM(held_pages.shape, held_pages.dtype)] * (stage == "stored"),
        ],
        input_output_aliases=aliases,
        compiler_params=pltpu.CompilerParams(vmem_limit_bytes=VMEM_LIMIT),
        name="attend_" + stage,
        cost_estimate=pl.CostEstimate(flops=4 * pairs * HEAD_SIZE, bytes_accessed=10_000_000, transcendentals=pairs),
    )(*operands)


def shards(
    queries, current_keys, current_values, stored_keys, stored_values, remap_table, block_table
):
    rows = queries.shape[0]
    kv_local = current_keys.shape[1] // HEAD_SIZE
    per_group = queries.shape[1] // (kv_local * HEAD_SIZE)
    owners = lax.axis_size("seq")
    me = lax.axis_index("seq")
    right = [(i, (i + 1) % owners) for i in range(owners)]
    left = [(i, (i - 1) % owners) for i in range(owners)]

    def packed(g):
        columns = slice(g * HEAD_SIZE, (g + 1) * HEAD_SIZE)
        stored = jnp.stack([stored_keys[:, :, columns], stored_values[:, :, columns]]).transpose(2, 0, 1, 3)
        current = jnp.stack([current_keys[:, columns], current_values[:, columns]])[None]
        return jnp.concatenate([stored, current])

    own = [packed(g) for g in range(kv_local)]
    slots = lax.dynamic_slice_in_dim(block_table.reshape(owners, owners), me, 1, 1)[:, 0]

    q = rotate_queries(queries, remap_table, kv_local, per_group)
    rightward, leftward = list(own), list(own)
    state = None
    for hop in range(1, owners // 2 + 1):
        held = [[rightward[g], leftward[g]] for g in range(kv_local)]
        if state is not None:
            for g in range(kv_local):
                rightward[g], leftward[g], _ = lax.optimization_barrier((rightward[g], leftward[g], state[1]))
        if hop < owners // 2:
            for g in range(kv_local):
                rightward[g] = lax.ppermute(rightward[g], "seq", right)
                leftward[g] = lax.ppermute(leftward[g], "seq", left)
        else:
            far_stored, far_current = [], []
            for g in range(kv_local):
                chunk, pairs, shift = (rightward[g], right, 1) if g % 2 == 0 else (leftward[g], left, -1)
                far_stored.append(lax.ppermute(chunk[:PRIOR_SEGMENTS], "seq", pairs))
                late = [(i, (i + shift) % owners) for i in range(owners) if (i + shift) % owners >= hop]
                far_current.append(lax.ppermute(chunk[PRIOR_SEGMENTS:], "seq", late))
        if state is None:
            state = attend(q, [[c] for c in own], [], (0,), owners, "first")
        else:
            state = attend(q, held, state, (hop - 1, owners - hop + 1), owners, "middle")
    *state, _, page_keys, page_values = attend(
        q, [[c] for c in far_stored], state, (owners // 2,), owners, "stored", slots
    )
    *_, attended = attend(q, [[c] for c in far_current], state[:2], (owners // 2,), owners, "finish")
    return (attended, page_keys, page_values)


def solution(mesh):
    in_specs = (
        P(("groups", "seq"), "head"),
        P(("groups", "seq"), "head"),
        P(("groups", "seq"), "head"),
        P(("groups", "seq"), None, "head"),
        P(("groups", "seq"), None, "head"),
        P(None, ("groups", "seq")),
        P("groups"),
    )
    out_specs = (
        P(("groups", "seq"), "head"),
        P("head", ("groups", "seq"), None),
        P("head", ("groups", "seq"), None),
    )
    return jax.shard_map(shards, mesh=mesh, in_specs=in_specs, out_specs=out_specs, check_vma=False)
```

```python
import functools
import math

import jax
import jax.numpy as jnp
from jax import lax
from jax.experimental import pallas as pl
from jax.experimental.pallas import tpu as pltpu
from jax.sharding import PartitionSpec as P


HEAD_SIZE = 128
PRIOR_SEGMENTS = 2
PAGE_TOKENS = 16
QBLK = 64

rope_base = 1000000.0
masked_value = -1e30
EXP2_SCALE = math.log2(math.e) / math.sqrt(HEAD_SIZE)

ONES = 16
WHOLE = pl.BlockSpec(memory_space=pltpu.VMEM)
VMEM_LIMIT = 14 * 1024 * 1024


def rotate_kernel(cos_ref, sin_ref, query_ref, out_ref, wide_cos, wide_sin):
    kv_local, kinds, per_group, _, _ = out_ref.shape
    for kind in range(kinds):
        wide_cos[kind] = jnp.concatenate([cos_ref[kind], cos_ref[kind]], -1)
        wide_sin[kind] = jnp.concatenate([-sin_ref[kind], sin_ref[kind]], -1)

    @pl.loop(0, per_group)
    def of_head(r):
        for g in range(kv_local):
            column = pl.multiple_of((g * per_group + r) * HEAD_SIZE, HEAD_SIZE)
            x = query_ref[:, pl.ds(column, HEAD_SIZE)].astype(jnp.float32)
            swapped = pltpu.roll(x, HEAD_SIZE // 2, 1)
            for kind in range(kinds):
                out_ref[g, kind, r] = (x * wide_cos[kind] + swapped * wide_sin[kind]).astype(jnp.bfloat16)


def rotate_queries(queries, remap_table, kv_local, per_group):
    rows = queries.shape[0]
    half = HEAD_SIZE // 2
    positions = (
        jnp.repeat(remap_table, QBLK, axis=1)
        + (jnp.arange(rows, dtype=jnp.int32) % QBLK)[None, :]
    )
    frequency = rope_base ** (-2.0 * jnp.arange(half, dtype=jnp.float32) / HEAD_SIZE)
    angles = positions.astype(jnp.float32)[:, :, None] * frequency[None, None, :]
    return pl.pallas_call(
        rotate_kernel,
        in_specs=[WHOLE] * 3,
        out_specs=WHOLE,
        out_shape=jax.ShapeDtypeStruct((kv_local, 3, per_group, rows, HEAD_SIZE), jnp.bfloat16),
        scratch_shapes=[pltpu.VMEM((3, rows, HEAD_SIZE), jnp.float32)] * 2,
        compiler_params=pltpu.CompilerParams(vmem_limit_bytes=16 * 1024 * 1024),
        name="rotate",
        cost_estimate=pl.CostEstimate(flops=1_000_000_000, bytes_accessed=4_000_000, transcendentals=0),
    )(jnp.cos(angles), jnp.sin(angles), queries)


def score(g, r, parts, max_ref, score_ref):
    best = []
    for n, (k, q, mask) in enumerate(parts):
        s = lax.dot_general(k, q, (((1,), (1,)), ((), ())), preferred_element_type=jnp.float32)
        if mask is not None:
            s = jnp.where(mask, s, masked_value)
        score_ref[n * s.shape[0] : (n + 1) * s.shape[0]] = s
        best.append(jnp.max(s, axis=0, keepdims=True))
    old_max = max_ref[g, r]
    new_max = functools.reduce(jnp.maximum, best, old_max)
    max_ref[g, r] = new_max
    return new_max, jnp.exp2((old_max - new_max) * EXP2_SCALE)


def weigh(keys, new_max, score_ref, weight_ref):
    weight_ref[:keys] = jnp.exp2((score_ref[:keys] - new_max) * EXP2_SCALE).astype(jnp.bfloat16)


def collect(g, r, keys, values, factor, weight_ref, acc_ref):
    product = jnp.dot(values, weight_ref[:keys], preferred_element_type=jnp.float32)
    acc_ref[g, r] = acc_ref[g, r] * factor + product


def put_page(page_ref, g, kv_ref, place, source):
    for which in range(2):
        page_ref[g, which, source] = kv_ref[
            PRIOR_SEGMENTS - 1, which, pl.ds(pl.multiple_of(place * PAGE_TOKENS, PAGE_TOKENS), PAGE_TOKENS), :
        ]


def attend_kernel(hops, owners, kv_local, stage, *refs):
    count = len(hops)
    if stage == "stored":
        slot_ref, refs = refs[0], refs[1:]
    q_ref, refs = refs[0], refs[1:]
    kv_refs, refs = refs[: kv_local * count], refs[kv_local * count :]
    _, _, per_group, rows, _ = q_ref.shape
    if stage == "first":
        (acc_ref, max_ref, page_ref), refs = refs[:3], refs[3:]
    elif stage == "middle":
        (acc_ref, max_ref, page_ref), refs = refs[:3], refs[6:]
    elif stage == "stored":
        (acc_ref, max_ref, page_ref), refs = refs[:3], refs[6:]
        (page_key_ref, page_value_ref, *refs, place_ref) = refs
    else:
        (acc_ref, max_ref), refs = refs[:2], refs[4:]
        (out_ref, *refs) = refs
    turned_ref, score_refs, weight_refs = refs[0], refs[1 : 1 + kv_local], refs[1 + kv_local :]
    me = lax.axis_index("seq")
    sources = [lax.rem(me + owners - hop, owners) for hop in hops]
    held = {
        "first": range(PRIOR_SEGMENTS + 1),
        "middle": range(PRIOR_SEGMENTS + 1),
        "stored": range(PRIOR_SEGMENTS),
        "finish": range(PRIOR_SEGMENTS, PRIOR_SEGMENTS + 1),
    }[stage]
    base = held[0]

    if stage == "first":
        acc_ref[...] = jnp.zeros_like(acc_ref)
        max_ref[...] = jnp.full_like(max_ref, masked_value)
    for g in range(kv_local):
        for c in range(count):
            kv = kv_refs[g * count + c]
            if stage != "finish":
                put_page(page_ref, g, kv, me, sources[c])
            for segment in held:
                turned_ref[g * count + c, segment, :HEAD_SIZE] = kv[segment - base, 1].T
                turned_ref[g * count + c, segment, HEAD_SIZE:] = jnp.ones((ONES, rows), jnp.bfloat16)

    def run(which, segments, mask=None):
        keys = len(which) * len(segments) * rows

        def parts(g, r):
            return [
                (kv_refs[g * count + c][segment - base, 0], q_ref[g, kind, r], mask)
                for segment, kind in segments
                for c in which
            ]

        def values(g):
            return jnp.concatenate(
                [turned_ref[g * count + c, segment] for segment, _ in segments for c in which], axis=1
            )

        heads = range(kv_local)

        def step(r, carry):
            maxima, factors = carry
            for g in heads:
                collect(g, jnp.maximum(r - 1, 0), keys, values(g), factors[g], weight_refs[g], acc_ref)
            following = jnp.minimum(r + 1, per_group - 1)
            scored = []
            for g in heads:
                weigh(keys, maxima[g][0], score_refs[g], weight_refs[g])
                scored.append(score(g, following, parts(g, following), max_ref, score_refs[g]))
            return scored, [of_head[1] for of_head in maxima]

        for g in heads:
            weight_refs[g][:keys] = jnp.zeros((keys, rows), jnp.bfloat16)
        scored = [score(g, 0, parts(g, 0), max_ref, score_refs[g]) for g in heads]
        _, factors = lax.fori_loop(0, per_group, step, (scored, [jnp.ones((1, rows), jnp.float32) for _ in heads]))
        for g in heads:
            collect(g, per_group - 1, keys, values(g), factors[g], weight_refs[g], acc_ref)

    stored = [(n, 2 if n < PRIOR_SEGMENTS - 1 else 1) for n in range(PRIOR_SEGMENTS)]
    current = [(PRIOR_SEGMENTS, 0)]
    if stage != "finish":
        run(range(count), stored)
    if stage == "first":
        shape = (rows, rows)
        mask = lax.broadcasted_iota(jnp.int32, shape, 0) <= lax.broadcasted_iota(jnp.int32, shape, 1)
        run([0], current, mask)
    elif stage == "finish":

        @pl.when(sources[0] < me)
        def before():
            run([0], current)

        @pl.loop(0, per_group)
        def finish(r):
            for g in range(kv_local):
                column = pl.multiple_of((g * per_group + r) * HEAD_SIZE, HEAD_SIZE)
                out_ref[:, pl.ds(column, HEAD_SIZE)] = (
                    (acc_ref[g, r, :HEAD_SIZE] / acc_ref[g, r, HEAD_SIZE : HEAD_SIZE + 1]).T.astype(jnp.bfloat16)
                )

    elif stage == "middle":
        @pl.when((sources[0] < me) & (sources[1] > me))
        def one():
            run([0], current)

        @pl.when(sources[1] < me)
        def two():
            run([0, 1], current)

    else:
        for source in range(owners):
            for g in range(kv_local):
                for which in range(2):
                    place_ref[g, which, slot_ref[source]] = page_ref[g, which, source]
        for g in range(kv_local):
            for which, ref in enumerate((page_key_ref, page_value_ref)):
                tokens = place_ref[g, which].astype(jnp.float32)
                for t in range(PAGE_TOKENS):
                    ref[g, :, t * HEAD_SIZE : (t + 1) * HEAD_SIZE] = tokens[:, t, :].astype(jnp.bfloat16)


def attend(q, chunks, state, hops, owners, stage, slots=None):
    kv_local, _, per_group, rows, _ = q.shape
    flat = [c for of_head in chunks for c in of_head]
    pages = rows // PAGE_TOKENS
    operands = [q, *flat] if slots is None else [slots, q, *flat]
    aliases = {len(operands) + n: n for n in range(len(state))}
    operands += state
    states = [
        jax.ShapeDtypeStruct((kv_local, per_group, n, rows), jnp.float32) for n in (HEAD_SIZE + ONES, 1)
    ]
    held_pages = jax.ShapeDtypeStruct((kv_local, 2, pages, PAGE_TOKENS, HEAD_SIZE), jnp.bfloat16)
    page = jax.ShapeDtypeStruct((kv_local, pages, PAGE_TOKENS * HEAD_SIZE), jnp.bfloat16)
    if stage == "finish":
        out_shape = [*states, jax.ShapeDtypeStruct((rows, kv_local * per_group * HEAD_SIZE), jnp.bfloat16)]
    elif stage == "stored":
        out_shape = [*states, held_pages, page, page]
    else:
        out_shape = [
            *states,
            held_pages,
        ]
    segments = {"first": 3, "middle": 3, "stored": 2, "finish": 1}[stage]
    keys = len(hops) * rows * (1 if stage == "finish" else PRIOR_SEGMENTS)
    pairs = len(hops) * kv_local * per_group * rows * rows * segments
    return pl.pallas_call(
        functools.partial(attend_kernel, hops, owners, kv_local, stage),
        in_specs=[pl.BlockSpec(memory_space=pltpu.SMEM)] * (slots is not None) + [WHOLE] * (len(operands) - (slots is not None)),
        out_specs=[WHOLE] * len(out_shape),
        out_shape=out_shape,
        scratch_shapes=[
            pltpu.VMEM((len(flat), PRIOR_SEGMENTS + 1, HEAD_SIZE + ONES, rows), jnp.bfloat16),
            *[pltpu.VMEM((keys, rows), t) for t in [jnp.float32] * kv_local + [jnp.bfloat16] * kv_local],
            *[pltpu.VMEM(held_pages.shape, held_pages.dtype)] * (stage == "stored"),
        ],
        input_output_aliases=aliases,
        compiler_params=pltpu.CompilerParams(vmem_limit_bytes=VMEM_LIMIT),
        name="attend_" + stage,
        cost_estimate=pl.CostEstimate(flops=4 * pairs * HEAD_SIZE, bytes_accessed=10_000_000, transcendentals=pairs),
    )(*operands)


def shards(
    queries, current_keys, current_values, stored_keys, stored_values, remap_table, block_table
):
    rows = queries.shape[0]
    kv_local = current_keys.shape[1] // HEAD_SIZE
    per_group = queries.shape[1] // (kv_local * HEAD_SIZE)
    owners = lax.axis_size("seq")
    me = lax.axis_index("seq")
    right = [(i, (i + 1) % owners) for i in range(owners)]
    left = [(i, (i - 1) % owners) for i in range(owners)]

    def packed(g):
        columns = slice(g * HEAD_SIZE, (g + 1) * HEAD_SIZE)
        stored = jnp.stack([stored_keys[:, :, columns], stored_values[:, :, columns]]).transpose(2, 0, 1, 3)
        current = jnp.stack([current_keys[:, columns], current_values[:, columns]])[None]
        return jnp.concatenate([stored, current])

    own = [packed(g) for g in range(kv_local)]
    slots = lax.dynamic_slice_in_dim(block_table.reshape(owners, owners), me, 1, 1)[:, 0]

    q = rotate_queries(queries, remap_table, kv_local, per_group)
    q, slots = lax.optimization_barrier((q, slots))
    rightward, leftward = list(own), list(own)
    state = None
    for hop in range(1, owners // 2 + 1):
        held = [[rightward[g], leftward[g]] for g in range(kv_local)]
        if state is not None:
            for g in range(kv_local):
                rightward[g], leftward[g], _ = lax.optimization_barrier((rightward[g], leftward[g], state[1]))
        if hop < owners // 2:
            for g in range(kv_local):
                rightward[g] = lax.ppermute(rightward[g], "seq", right)
                leftward[g] = lax.ppermute(leftward[g], "seq", left)
        else:
            far_stored, far_current = [], []
            for g in range(kv_local):
                chunk, pairs, shift = (rightward[g], right, 1) if g % 2 == 0 else (leftward[g], left, -1)
                far_stored.append(lax.ppermute(chunk[:PRIOR_SEGMENTS], "seq", pairs))
                late = [(i, (i + shift) % owners) for i in range(owners) if (i + shift) % owners >= hop]
                far_current.append(lax.ppermute(chunk[PRIOR_SEGMENTS:], "seq", late))
        if state is None:
            state = attend(q, [[c] for c in own], [], (0,), owners, "first")
        else:
            state = attend(q, held, state, (hop - 1, owners - hop + 1), owners, "middle")
    *state, _, page_keys, page_values = attend(
        q, [[c] for c in far_stored], state, (owners // 2,), owners, "stored", slots
    )
    *_, attended = attend(q, [[c] for c in far_current], state[:2], (owners // 2,), owners, "finish")
    return (attended, page_keys, page_values)


def solution(mesh):
    in_specs = (
        P(("groups", "seq"), "head"),
        P(("groups", "seq"), "head"),
        P(("groups", "seq"), "head"),
        P(("groups", "seq"), None, "head"),
        P(("groups", "seq"), None, "head"),
        P(None, ("groups", "seq")),
        P("groups"),
    )
    out_specs = (
        P(("groups", "seq"), "head"),
        P("head", ("groups", "seq"), None),
        P("head", ("groups", "seq"), None),
    )
    return jax.shard_map(shards, mesh=mesh, in_specs=in_specs, out_specs=out_specs, check_vma=False)
```

```python
import functools
import math

import jax
import jax.numpy as jnp
from jax import lax
from jax.experimental import pallas as pl
from jax.experimental.pallas import tpu as pltpu
from jax.sharding import PartitionSpec as P


HEAD_SIZE = 128
PRIOR_SEGMENTS = 2
PAGE_TOKENS = 16
QBLK = 64

rope_base = 1000000.0
masked_value = -1e30
EXP2_SCALE = math.log2(math.e) / math.sqrt(HEAD_SIZE)

ONES = 16
WHOLE = pl.BlockSpec(memory_space=pltpu.VMEM)
VMEM_LIMIT = 14 * 1024 * 1024


def rotate_kernel(cos_ref, sin_ref, query_ref, out_ref, wide_cos, wide_sin):
    kv_local, kinds, per_group, _, _ = out_ref.shape
    for kind in range(kinds):
        wide_cos[kind] = jnp.concatenate([cos_ref[kind], cos_ref[kind]], -1)
        wide_sin[kind] = jnp.concatenate([-sin_ref[kind], sin_ref[kind]], -1)

    @pl.loop(0, per_group)
    def of_head(r):
        for g in range(kv_local):
            column = pl.multiple_of((g * per_group + r) * HEAD_SIZE, HEAD_SIZE)
            x = query_ref[:, pl.ds(column, HEAD_SIZE)].astype(jnp.float32)
            swapped = pltpu.roll(x, HEAD_SIZE // 2, 1)
            for kind in range(kinds):
                out_ref[g, kind, r] = (x * wide_cos[kind] + swapped * wide_sin[kind]).astype(jnp.bfloat16)


def rotate_queries(queries, remap_table, kv_local, per_group):
    rows = queries.shape[0]
    half = HEAD_SIZE // 2
    positions = (
        jnp.repeat(remap_table, QBLK, axis=1)
        + (jnp.arange(rows, dtype=jnp.int32) % QBLK)[None, :]
    )
    frequency = rope_base ** (-2.0 * jnp.arange(half, dtype=jnp.float32) / HEAD_SIZE)
    angles = positions.astype(jnp.float32)[:, :, None] * frequency[None, None, :]
    return pl.pallas_call(
        rotate_kernel,
        in_specs=[WHOLE] * 3,
        out_specs=WHOLE,
        out_shape=jax.ShapeDtypeStruct((kv_local, 3, per_group, rows, HEAD_SIZE), jnp.bfloat16),
        scratch_shapes=[pltpu.VMEM((3, rows, HEAD_SIZE), jnp.float32)] * 2,
        compiler_params=pltpu.CompilerParams(vmem_limit_bytes=16 * 1024 * 1024),
        name="rotate",
        cost_estimate=pl.CostEstimate(flops=1_000_000_000, bytes_accessed=4_000_000, transcendentals=0),
    )(jnp.cos(angles), jnp.sin(angles), queries)


def score(g, r, parts, max_ref, score_ref):
    best = []
    for n, (k, q, mask) in enumerate(parts):
        s = lax.dot_general(k, q, (((1,), (1,)), ((), ())), preferred_element_type=jnp.float32)
        if mask is not None:
            s = jnp.where(mask, s, masked_value)
        score_ref[n * s.shape[0] : (n + 1) * s.shape[0]] = s
        best.append(jnp.max(s, axis=0, keepdims=True))
    old_max = max_ref[g, r]
    new_max = functools.reduce(jnp.maximum, best, old_max)
    max_ref[g, r] = new_max
    return new_max, jnp.exp2((old_max - new_max) * EXP2_SCALE)


def weigh(keys, new_max, score_ref, weight_ref):
    weight_ref[:keys] = jnp.exp2((score_ref[:keys] - new_max) * EXP2_SCALE).astype(jnp.bfloat16)


def collect(g, r, keys, values, factor, weight_ref, acc_ref):
    product = jnp.dot(values, weight_ref[:keys], preferred_element_type=jnp.float32)
    acc_ref[g, r] = acc_ref[g, r] * factor + product


def put_page(page_ref, g, stored_ref, place, source):
    for which in range(2):
        page_ref[g, which, source] = stored_ref[
            g, PRIOR_SEGMENTS - 1, which, pl.ds(pl.multiple_of(place * PAGE_TOKENS, PAGE_TOKENS), PAGE_TOKENS), :
        ]


def attend_kernel(hops, owners, kv_local, stage, *refs):
    count = len(hops)
    if stage == "stored":
        slot_ref, refs = refs[0], refs[1:]
    q_ref, refs = refs[0], refs[1:]
    stored_refs = current_refs = None
    if stage != "finish":
        stored_refs, refs = refs[:count], refs[count:]
    if stage != "stored":
        current_refs, refs = refs[:count], refs[count:]
    _, _, per_group, rows, _ = q_ref.shape
    if stage == "first":
        (acc_ref, max_ref, page_ref), refs = refs[:3], refs[3:]
    elif stage == "middle":
        (acc_ref, max_ref, page_ref), refs = refs[:3], refs[6:]
    elif stage == "stored":
        (acc_ref, max_ref, page_ref), refs = refs[:3], refs[6:]
        (page_key_ref, page_value_ref, *refs, place_ref) = refs
    else:
        (acc_ref, max_ref), refs = refs[:2], refs[4:]
        (out_ref, *refs) = refs
    turned_ref, score_refs, weight_refs = refs[0], refs[1 : 1 + kv_local], refs[1 + kv_local :]
    me = lax.axis_index("seq")
    sources = [lax.rem(me + owners - hop, owners) for hop in hops]
    held = {
        "first": range(PRIOR_SEGMENTS + 1),
        "middle": range(PRIOR_SEGMENTS + 1),
        "stored": range(PRIOR_SEGMENTS),
        "finish": range(PRIOR_SEGMENTS, PRIOR_SEGMENTS + 1),
    }[stage]

    def piece(g, c, segment, which):
        if segment < PRIOR_SEGMENTS:
            return stored_refs[c][g, segment, which]
        return current_refs[c][g, 0, which]

    if stage == "first":
        acc_ref[...] = jnp.zeros_like(acc_ref)
        max_ref[...] = jnp.full_like(max_ref, masked_value)
    for g in range(kv_local):
        for c in range(count):
            if stage != "finish":
                put_page(page_ref, g, stored_refs[c], me, sources[c])
            for segment in held:
                turned_ref[g * count + c, segment, :HEAD_SIZE] = piece(g, c, segment, 1).T
                turned_ref[g * count + c, segment, HEAD_SIZE:] = jnp.ones((ONES, rows), jnp.bfloat16)

    def run(which, segments, mask=None):
        keys = len(which) * len(segments) * rows

        def parts(g, r):
            return [
                (piece(g, c, segment, 0), q_ref[g, kind, r], mask)
                for segment, kind in segments
                for c in which
            ]

        def values(g):
            return jnp.concatenate(
                [turned_ref[g * count + c, segment] for segment, _ in segments for c in which], axis=1
            )

        heads = range(kv_local)

        def step(r, carry):
            maxima, factors = carry
            for g in heads:
                collect(g, jnp.maximum(r - 1, 0), keys, values(g), factors[g], weight_refs[g], acc_ref)
            following = jnp.minimum(r + 1, per_group - 1)
            scored = []
            for g in heads:
                weigh(keys, maxima[g][0], score_refs[g], weight_refs[g])
                scored.append(score(g, following, parts(g, following), max_ref, score_refs[g]))
            return scored, [of_head[1] for of_head in maxima]

        for g in heads:
            weight_refs[g][:keys] = jnp.zeros((keys, rows), jnp.bfloat16)
        scored = [score(g, 0, parts(g, 0), max_ref, score_refs[g]) for g in heads]
        _, factors = lax.fori_loop(0, per_group, step, (scored, [jnp.ones((1, rows), jnp.float32) for _ in heads]))
        for g in heads:
            collect(g, per_group - 1, keys, values(g), factors[g], weight_refs[g], acc_ref)

    stored = [(n, 2 if n < PRIOR_SEGMENTS - 1 else 1) for n in range(PRIOR_SEGMENTS)]
    current = [(PRIOR_SEGMENTS, 0)]
    if stage != "finish":
        run(range(count), stored)
    if stage == "first":
        shape = (rows, rows)
        mask = lax.broadcasted_iota(jnp.int32, shape, 0) <= lax.broadcasted_iota(jnp.int32, shape, 1)
        run([0], current, mask)
    elif stage == "finish":

        @pl.when(sources[0] < me)
        def before():
            run([0], current)

        @pl.loop(0, per_group)
        def finish(r):
            for g in range(kv_local):
                column = pl.multiple_of((g * per_group + r) * HEAD_SIZE, HEAD_SIZE)
                out_ref[:, pl.ds(column, HEAD_SIZE)] = (
                    (acc_ref[g, r, :HEAD_SIZE] / acc_ref[g, r, HEAD_SIZE : HEAD_SIZE + 1]).T.astype(jnp.bfloat16)
                )

    elif stage == "middle":
        @pl.when((sources[0] < me) & (sources[1] > me))
        def one():
            run([0], current)

        @pl.when(sources[1] < me)
        def two():
            run([0, 1], current)

    else:
        for source in range(owners):
            for g in range(kv_local):
                for which in range(2):
                    place_ref[g, which, slot_ref[source]] = page_ref[g, which, source]
        for g in range(kv_local):
            for which, ref in enumerate((page_key_ref, page_value_ref)):
                tokens = place_ref[g, which].astype(jnp.float32)
                for t in range(PAGE_TOKENS):
                    ref[g, :, t * HEAD_SIZE : (t + 1) * HEAD_SIZE] = tokens[:, t, :].astype(jnp.bfloat16)


def attend(q, chunks, state, hops, owners, stage, slots=None):
    kv_local, _, per_group, rows, _ = q.shape
    flat = list(chunks)
    pages = rows // PAGE_TOKENS
    operands = [q, *flat] if slots is None else [slots, q, *flat]
    aliases = {len(operands) + n: n for n in range(len(state))}
    operands += state
    states = [
        jax.ShapeDtypeStruct((kv_local, per_group, n, rows), jnp.float32) for n in (HEAD_SIZE + ONES, 1)
    ]
    held_pages = jax.ShapeDtypeStruct((kv_local, 2, pages, PAGE_TOKENS, HEAD_SIZE), jnp.bfloat16)
    page = jax.ShapeDtypeStruct((kv_local, pages, PAGE_TOKENS * HEAD_SIZE), jnp.bfloat16)
    if stage == "finish":
        out_shape = [*states, jax.ShapeDtypeStruct((rows, kv_local * per_group * HEAD_SIZE), jnp.bfloat16)]
    elif stage == "stored":
        out_shape = [*states, held_pages, page, page]
    else:
        out_shape = [
            *states,
            held_pages,
        ]
    segments = {"first": 3, "middle": 3, "stored": 2, "finish": 1}[stage]
    keys = len(hops) * rows * (1 if stage == "finish" else PRIOR_SEGMENTS)
    pairs = len(hops) * kv_local * per_group * rows * rows * segments
    return pl.pallas_call(
        functools.partial(attend_kernel, hops, owners, kv_local, stage),
        in_specs=[pl.BlockSpec(memory_space=pltpu.SMEM)] * (slots is not None) + [WHOLE] * (len(operands) - (slots is not None)),
        out_specs=[WHOLE] * len(out_shape),
        out_shape=out_shape,
        scratch_shapes=[
            pltpu.VMEM((kv_local * len(hops), PRIOR_SEGMENTS + 1, HEAD_SIZE + ONES, rows), jnp.bfloat16),
            *[pltpu.VMEM((keys, rows), t) for t in [jnp.float32] * kv_local + [jnp.bfloat16] * kv_local],
            *[pltpu.VMEM(held_pages.shape, held_pages.dtype)] * (stage == "stored"),
        ],
        input_output_aliases=aliases,
        compiler_params=pltpu.CompilerParams(vmem_limit_bytes=VMEM_LIMIT),
        name="attend_" + stage,
        cost_estimate=pl.CostEstimate(flops=4 * pairs * HEAD_SIZE, bytes_accessed=10_000_000, transcendentals=pairs),
    )(*operands)


def shards(
    queries, current_keys, current_values, stored_keys, stored_values, remap_table, block_table
):
    rows = queries.shape[0]
    kv_local = current_keys.shape[1] // HEAD_SIZE
    per_group = queries.shape[1] // (kv_local * HEAD_SIZE)
    owners = lax.axis_size("seq")
    me = lax.axis_index("seq")
    right = [(i, (i + 1) % owners) for i in range(owners)]
    left = [(i, (i - 1) % owners) for i in range(owners)]

    def by_head(keys, values, segments):
        both = jnp.stack([a.reshape(rows, segments, kv_local, HEAD_SIZE) for a in (keys, values)])
        return both.transpose(3, 2, 0, 1, 4)

    own_stored = by_head(stored_keys, stored_values, PRIOR_SEGMENTS)
    own_current = by_head(current_keys, current_values, 1)
    slots = lax.dynamic_slice_in_dim(block_table.reshape(owners, owners), me, 1, 1)[:, 0]

    q = rotate_queries(queries, remap_table, kv_local, per_group)
    q, slots = lax.optimization_barrier((q, slots))
    half = owners // 2
    useful_right = lambda hop: [(i, i + 1) for i in range(owners - 1) if i - hop + 1 >= 0]
    useful_left = lambda hop: [
        ((s - hop + 1) % owners, (s - hop) % owners) for s in range(owners) if s + half < owners
    ]
    stored = [own_stored, own_stored]
    current = [own_current, own_current]
    state = None
    for hop in range(1, half + 1):
        held = [*stored, *current]
        if state is not None:
            *stored, _ = lax.optimization_barrier((*stored, state[1]))
            *current, _ = lax.optimization_barrier((*current, state[1]))
        if hop < half:
            stored = [lax.ppermute(a, "seq", pairs) for a, pairs in zip(stored, (right, left))]
            current = [
                lax.ppermute(a, "seq", pairs) for a, pairs in zip(current, (useful_right(hop), useful_left(hop)))
            ]
        else:
            cut = [slice(0, kv_local // 2), slice(kv_local // 2, kv_local)]
            far_stored = jnp.concatenate(
                [lax.ppermute(a[at], "seq", pairs) for a, at, pairs in zip(stored, cut, (right, left))]
            )
            far_current = jnp.concatenate(
                [
                    lax.ppermute(a[at], "seq", pairs)
                    for a, at, pairs in zip(current, cut, (useful_right(hop), useful_left(hop)))
                ]
            )
        if state is None:
            state = attend(q, [own_stored, own_current], [], (0,), owners, "first")
        else:
            state = attend(q, held, state, (hop - 1, owners - hop + 1), owners, "middle")
    *state, _, page_keys, page_values = attend(q, [far_stored], state, (half,), owners, "stored", slots)
    *_, attended = attend(q, [far_current], state[:2], (half,), owners, "finish")
    return (attended, page_keys, page_values)


def solution(mesh):
    in_specs = (
        P(("groups", "seq"), "head"),
        P(("groups", "seq"), "head"),
        P(("groups", "seq"), "head"),
        P(("groups", "seq"), None, "head"),
        P(("groups", "seq"), None, "head"),
        P(None, ("groups", "seq")),
        P("groups"),
    )
    out_specs = (
        P(("groups", "seq"), "head"),
        P("head", ("groups", "seq"), None),
        P("head", ("groups", "seq"), None),
    )
    return jax.shard_map(shards, mesh=mesh, in_specs=in_specs, out_specs=out_specs, check_vma=False)
```
